32 devices in a mesh: ka: 16 (over z, y, core), ga: 2 (over x).
Axes of the slice: x: 2, y: 2, z: 4, core: 2. Of those that a mesh axis runs over, the one named last changes fastest.
Arguments:
- coeffs: bfloat16 [16, 240, 2, 64, 128], P('ka', 'ga'), may hold values from -0.44921875 to 0.44921875
- neighbour: int32 [16, 3], P('ka'), may hold values from 0 to 15, as said below
- shift_id: int32 [16, 3], P('ka'), may hold values from 0 to 7
- block_map: int32 [8, 240], replicated, may hold values from 0 to 239, as said below
Outputs:
- intersection: float32 [16, 3, 2, 64, 64], P('ka', None, None, 'ga')
The draws below stay inside these ranges and needn't reach their ends.
Inputs may be any that keep to these rules, and one draw needn't show every extreme that they name: `neighbour`: the k-points are numbered helically. The three columns of row k hold (k + 1) mod 16, (k + 4) mod 16 and (k + 8) mod 16, in an order drawn for each row. `block_map`: each row is a permutation of the 240 blocks. Block j lies in G-slice j // 120. In every row, each G-slice receives exactly 20 of its blocks from one other G-slice, exactly 10 from each of the remaining other G-slices, and the rest from itself.
All inputs are finite; a program needn't handle non-finite values.
Results may differ from the reference program's by a relative error of at most 0.0003.
Values may be sent and summed in bfloat16 or wider, within the bound.
A program may use at most 128 MiB of HBM per device.

```python
import jax
import jax.numpy as jnp
from jax import lax

NB = 64
NBV = 3
NSHIFT = 8
K_DEV = 1
KPTS = 16
MZ = 4
NBLK = 240
BLK_SL = 120
CAP = 20
N_KA = 16
N_GA = 2


def column_order(one_key):
    return jax.random.permutation(one_key, 3).astype(jnp.int32)


def draw_neighbour(key, part):
    total = K_DEV * N_KA
    points = jnp.arange(total, dtype=jnp.int32)
    z_step = jnp.mod(points + 1, total)
    y_step = jnp.mod(points + MZ, total)
    x_step = jnp.mod(points + total // 2, total)
    stacked = jnp.stack([z_step, y_step, x_step], axis=1).astype(jnp.int32)
    orders = jax.vmap(column_order)(jax.random.split(jax.random.fold_in(key, 17), total))
    return jnp.take_along_axis(stacked, orders, axis=1).astype(jnp.int32)


def row_shuffle(one_key):
    return jax.random.permutation(one_key, BLK_SL).astype(jnp.int32)


def one_map(key):
    keys = jax.random.split(key, 3)
    lighter = CAP // 2
    heavy = jax.random.randint(keys[0], (), 1, N_GA, dtype=jnp.int32)
    rows = jnp.arange(N_GA, dtype=jnp.int32)[:, None]
    cols = jnp.arange(BLK_SL, dtype=jnp.int32)[None, :]
    self_count = BLK_SL - CAP - (N_GA - 2) * lighter
    remain = jnp.maximum(cols - self_count - CAP, 0) // lighter
    other_step = jnp.where(remain + 1 < heavy, remain + 1, remain + 2)
    offset = jnp.where(cols < self_count, 0, jnp.where(cols < self_count + CAP, heavy, other_step))
    labels = jnp.mod(rows + offset, N_GA).astype(jnp.int32)
    shuffles = jax.vmap(row_shuffle)(jax.random.split(keys[1], N_GA))
    labels = jnp.take_along_axis(labels, shuffles, axis=1).reshape(-1)
    grouped = jnp.argsort(labels, stable=True).astype(jnp.int32)
    inner = jax.vmap(row_shuffle)(jax.random.split(keys[2], N_GA))
    sources = (jnp.arange(N_GA, dtype=jnp.int32)[:, None] * BLK_SL + inner).reshape(-1)
    return jnp.zeros((N_GA * BLK_SL,), jnp.int32).at[grouped].set(sources)


def draw_block_map(key, part):
    keys = jax.random.split(key, NSHIFT)
    return jax.vmap(one_map)(keys).astype(jnp.int32)


def place_ends(values, own_key, least, top_value):
    place = [jax.random.randint(jax.random.fold_in(own_key, axis), (), 0, length) for axis, length in enumerate(values.shape)]
    main_axis = values.shape.index(max(values.shape))
    beside = place[:main_axis] + [(place[main_axis] + 1) % values.shape[main_axis]] + place[main_axis + 1:]
    return values.at[tuple(place)].set(least).at[tuple(beside)].set(top_value)


def block_scale(own_key, shape, pieces, smallest, largest):
    factor_of = 1.0
    for position, parts in pieces:
        steps = jax.random.uniform(jax.random.fold_in(jax.random.fold_in(own_key, 6), position), (parts,), jnp.float32, smallest / len(pieces), largest / len(pieces))
        factor_of = factor_of * jnp.repeat(jnp.exp(steps), shape[position] // parts).reshape((-1,) + (1,) * (len(shape) - 1 - position))
    return factor_of


def gaussian(key, extent, deviation, bound, cuts=(), held_as=jnp.bfloat16):
    loudness = block_scale(key, extent, cuts, -0.22, 0.18) if cuts else 1.0
    entries = jax.random.normal(key, extent, jnp.float32) * deviation * loudness
    return jnp.minimum(jnp.maximum(entries, -bound), bound).astype(held_as)


def setup_inputs(seed: int = 0) -> dict:
    arg_keys = jax.random.split(jax.random.key(seed), 5)
    coeffs = gaussian(arg_keys[0], (KPTS, NBLK, 2, NB, 128), 0.0755, 0.44921875, ((0, 16), (1, 2)))
    neighbour = draw_neighbour(jax.random.fold_in(arg_keys[4], 71), 0)
    shift_id = place_ends(jax.random.randint(arg_keys[2], (KPTS, NBV), 0, NSHIFT), jax.random.fold_in(arg_keys[2], 1), 0, NSHIFT - 1).astype(jnp.int32)
    block_map = draw_block_map(jax.random.fold_in(arg_keys[4], 71), 0)
    return dict(coeffs=coeffs, neighbour=neighbour, shift_id=shift_id, block_map=block_map)


def pair_product(left, right):
    return jnp.einsum("jmw,jnw->mn", left, right, precision=lax.Precision.HIGHEST)


def reference(coeffs, neighbour, shift_id, block_map):
    bra_points = (jnp.arange(KPTS * NBV, dtype=jnp.int32) // NBV).astype(jnp.int32)
    ket_points = neighbour.reshape(-1).astype(jnp.int32)
    shifts_flat = shift_id.reshape(-1).astype(jnp.int32)

    def one_pair(inputs):
        bra_point, ket_point, shift_row = inputs
        bra = coeffs[bra_point].astype(jnp.float32)
        ket = jnp.take(coeffs[ket_point], block_map[shift_row], axis=0).astype(jnp.float32)
        real_part = pair_product(bra[:, 0], ket[:, 0]) + pair_product(bra[:, 1], ket[:, 1])
        imag_part = pair_product(bra[:, 0], ket[:, 1]) - pair_product(bra[:, 1], ket[:, 0])
        return jnp.stack([real_part, imag_part])

    result = lax.map(one_pair, (bra_points, ket_points, shifts_flat))
    return result.reshape(KPTS, NBV, 2, NB, NB)
```

```python
import functools

import jax
import jax.numpy as jnp
from jax import lax
from jax.sharding import PartitionSpec as P
from jax.experimental import pallas as pl
from jax.experimental.pallas import tpu as pltpu

CHUNKS = 4


def shifted(block, axis, distance):
    devices = range(lax.axis_size(axis))
    route = [((i - distance) % len(devices), i) for i in devices]
    return lax.ppermute(block, axis, route)


def complex_intersection(bra_real, bra_imag, ket_real, ket_imag, form):
    real_part = jnp.einsum(form, bra_real, ket_real, preferred_element_type=jnp.float32)
    real_part = real_part + jnp.einsum(form, bra_imag, ket_imag, preferred_element_type=jnp.float32)
    imag_part = jnp.einsum(form, bra_real, ket_imag, preferred_element_type=jnp.float32)
    imag_part = imag_part - jnp.einsum(form, bra_imag, ket_real, preferred_element_type=jnp.float32)
    return jnp.stack([real_part, imag_part], axis=-3)


def slot_plan(
    home_slice, target_slice, sent_local, place_local, my_slice, slices, capacity, slab_blocks
):
    targets = jnp.arange(slices, dtype=jnp.int32)
    chosen = (home_slice == my_slice)[:, None, :] & (
        target_slice[:, None, :] == targets[None, :, None]
    )
    chosen = chosen & (targets != my_slice)[None, :, None]
    counted = jnp.cumsum(chosen.astype(jnp.int32), axis=2) - 1
    places = jnp.arange(capacity, dtype=jnp.int32)
    matched = (
        chosen[:, :, None, :] & (counted[:, :, None, :] == places[None, None, :, None])
    ).astype(jnp.int32)
    filled = jnp.sum(matched, axis=3)
    sent_block = jnp.sum(matched * sent_local[:, None, None, :], axis=3)
    where_to = jnp.sum(matched * place_local[:, None, None, :], axis=3) + (1 - filled) * slab_blocks
    pair_count = home_slice.shape[0]
    return (
        sent_block.reshape(pair_count, slices * capacity),
        where_to.reshape(pair_count, slices * capacity),
    )


def on_device(coeffs, neighbour, shift_id, block_map):
    k_local = coeffs.shape[0]
    slab_blocks = coeffs.shape[1]
    band_count = coeffs.shape[3]
    lane_width = coeffs.shape[4]
    vector_count = neighbour.shape[1]
    cycle_size = lax.axis_size("ka")
    slices = lax.axis_size("ga")
    my_cycle = lax.axis_index("ka")
    my_slice = lax.axis_index("ga")
    capacity = 2 * max(1, slab_blocks // 12)
    all_blocks = slab_blocks * slices
    pair_count = k_local * vector_count
    k_total = k_local * cycle_size
    row_points = min(16, k_total // 4)
    row_devices = row_points // k_local
    pad_spec = ((0, 0), (0, 1), (0, 0), (0, 0), (0, 0))
    row_point = shifted(coeffs, "ka", -1)
    row_source = jnp.mod(my_cycle + 1, cycle_size)
    plane_kets = shifted(coeffs, "ka", -row_devices)
    plane_source = jnp.mod(my_cycle + row_devices, cycle_size)
    opposite = shifted(coeffs, "ka", cycle_size // 2)
    targets_flat = neighbour.reshape(-1)
    shifts_flat = shift_id.reshape(-1)
    target_device = targets_flat // k_local
    target_lane = targets_flat - target_device * k_local
    ket_index = jnp.where(
        target_device == my_cycle,
        target_lane,
        jnp.where(
            target_device == row_source,
            k_local,
            jnp.where(
                target_device == plane_source,
                k_local + 1 + target_lane,
                2 * k_local + 1 + target_lane,
            ),
        ),
    )
    bra_index = jnp.arange(pair_count, dtype=jnp.int32) // vector_count
    picks = (
        shifts_flat[:, None] == jnp.arange(block_map.shape[0], dtype=jnp.int32)[None, :]
    ).astype(jnp.int32)
    relabel = jnp.sum(picks[:, :, None] * block_map[None, :, :], axis=1)
    dest_global = jnp.broadcast_to(jnp.arange(all_blocks, dtype=jnp.int32)[None, :], relabel.shape)
    source_slice = relabel // slab_blocks
    dest_slice = dest_global // slab_blocks
    source_local = relabel - source_slice * slab_blocks
    dest_local = dest_global - dest_slice * slab_blocks
    kets = jnp.pad(jnp.concatenate([coeffs, row_point, plane_kets, opposite], axis=0), pad_spec)
    own_source = lax.dynamic_slice_in_dim(relabel, my_slice * slab_blocks, slab_blocks, 1)
    self_place = jnp.where(
        own_source // slab_blocks == my_slice, own_source - my_slice * slab_blocks, slab_blocks
    )
    ket_self = kets[ket_index[:, None], self_place]
    ket_self = ket_self.reshape(k_local, vector_count, slab_blocks, 2, band_count, lane_width)
    local_terms = complex_intersection(
        coeffs[:, :, 0],
        coeffs[:, :, 1],
        ket_self[:, :, :, 0],
        ket_self[:, :, :, 1],
        "ksmw,kbsnw->kbmn",
    )
    sent_block, where_to = slot_plan(
        dest_slice, source_slice, dest_local, source_local, my_slice, slices, capacity, slab_blocks
    )
    payload = coeffs[bra_index[:, None], sent_block]
    owner = jnp.broadcast_to(ket_index[:, None], (pair_count, slices))
    blocks = lax.all_to_all(payload, "ga", split_axis=1, concat_axis=1, tiled=True)
    places_in = lax.all_to_all(where_to, "ga", split_axis=1, concat_axis=1, tiled=True)
    owners = lax.all_to_all(owner, "ga", split_axis=1, concat_axis=1, tiled=True)
    partner = kets[owners[:, 0][:, None], places_in]
    remote = complex_intersection(
        blocks[:, :, 0], blocks[:, :, 1], partner[:, :, 0], partner[:, :, 1], "ismw,isnw->imn"
    )
    summed_part = local_terms + remote.reshape(k_local, vector_count, 2, band_count, band_count)
    total = lax.psum(summed_part, "ga")
    row_count = band_count // slices
    return lax.dynamic_slice_in_dim(total, my_slice * row_count, row_count, 3)


def gather_kernel(count, index_ref, source_ref, out_ref, sems):
    def copy(i):
        return pltpu.make_async_copy(source_ref.at[index_ref[i]], out_ref.at[i], sems.at[i])

    def begin(i, carry):
        copy(i).start()
        return carry

    def finish(i, carry):
        copy(i).wait()
        return carry

    lax.fori_loop(0, count, begin, 0)
    lax.fori_loop(0, count, finish, 0)


def gather_blocks(index, source):
    count = index.shape[0]
    shape = (count,) + source.shape[1:]
    return pl.pallas_call(
        functools.partial(gather_kernel, count),
        out_shape=jax.ShapeDtypeStruct(shape, source.dtype),
        in_specs=[
            pl.BlockSpec(memory_space=pltpu.SMEM),
            pl.BlockSpec(memory_space=pl.ANY),
        ],
        out_specs=pl.BlockSpec(memory_space=pltpu.VMEM),
        scratch_shapes=[pltpu.SemaphoreType.DMA((count,))],
        name="gather_blocks",
        cost_estimate=pl.CostEstimate(flops=0, bytes_accessed=4 * source.dtype.itemsize * count * source[0].size, transcendentals=0),
    )(index, source)


def dot_kernel(edges, items, starts, *refs):
    count = len(starts)
    left_ref, right_ref = refs[0], refs[1]
    parts = refs[2 : 2 + count]
    out_ref, held, sems = refs[2 + count :]
    rows = held.shape[1] * held.shape[2]
    bands = held.shape[2]
    lanes = held.shape[3]
    copies = []
    for n, part in enumerate(parts):
        copy = pltpu.make_async_copy(part, held.at[pl.ds(starts[n], part.shape[0])], sems.at[n])
        copy.start()
        copies.append(copy)
    for copy in copies:
        copy.wait()
    unroll = 8 if items % 8 == 0 else 2

    for e in range(edges):
        def step(i, total):
            for u in range(0, unroll, 2):
                at = e * items + i * unroll + u
                left = jnp.concatenate(
                    [held[left_ref[at]].reshape(rows, lanes), held[left_ref[at + 1]].reshape(rows, lanes)], axis=1
                )
                right = jnp.concatenate(
                    [held[right_ref[at]].reshape(rows, lanes), held[right_ref[at + 1]].reshape(rows, lanes)], axis=1
                )
                total = total + lax.dot_general(
                    left, right, (((1,), (1,)), ((), ())), preferred_element_type=jnp.float32
                )
            return total

        total = lax.fori_loop(0, items // unroll, step, jnp.zeros((rows, rows), jnp.float32))
        out_ref[e, 0] = total[:bands, :bands] + total[bands:, bands:]
        out_ref[e, 1] = total[:bands, bands:] - total[bands:, :bands]


def dot_items(left, right, parts):
    edges, items = left.shape
    bands, lanes = parts[0].shape[2], parts[0].shape[3]
    starts, blocks = [], 0
    for part in parts:
        starts.append(blocks)
        blocks += part.shape[0]
    nbytes = blocks * parts[0][0].size * parts[0].dtype.itemsize
    return pl.pallas_call(
        functools.partial(dot_kernel, edges, items, tuple(starts)),
        out_shape=jax.ShapeDtypeStruct((edges, 2, bands, bands), jnp.float32),
        in_specs=[pl.BlockSpec(memory_space=pltpu.SMEM)] * 2
        + [pl.BlockSpec(memory_space=pl.ANY)] * len(parts),
        out_specs=pl.BlockSpec(memory_space=pltpu.VMEM),
        scratch_shapes=[
            pltpu.VMEM((blocks,) + parts[0].shape[1:], parts[0].dtype),
            pltpu.SemaphoreType.DMA((len(parts),)),
        ],
        compiler_params=pltpu.CompilerParams(vmem_limit_bytes=nbytes + 8 * 2**20),
        name="dot_items",
        cost_estimate=pl.CostEstimate(
            flops=edges * items * 2 * 4 * bands * bands * lanes, bytes_accessed=nbytes, transcendentals=0
        ),
    )(left.reshape(-1), right.reshape(-1), *parts)


def on_four_rows(coeffs, neighbour, shift_id, block_map):
    own = coeffs[0]
    slab = own.shape[0]
    points = lax.axis_size("ka")
    row = points // 4
    me = lax.axis_index("ka")
    mine = lax.axis_index("ga")
    column = jnp.mod(me, row)
    even = jnp.mod(column, 2) == 0
    capacity = 2 * max(1, slab // 12)

    down, up = [], []
    for k in range(points):
        z, i = k // row, k % row
        if i % 2 == 0 or z in (1, 2):
            down.append(((k + row) % points, k))
        if i % 2 == 1 or z in (0, 3):
            up.append(((k - row) % points, k))
    direct = [(k + 1, k) for k in range(points) if k % row < row - 1]
    around = [(k - (row - 1), k) for k in range(points) if k % row == row - 1]
    to_lower = [((k + row) % points, k) for k in range(points)]
    to_upper = [((k - row) % points, k) for k in range(points)]
    swap = [(0, 1), (1, 0)]

    def role_shift(step):
        return jnp.sum(jnp.where(neighbour[0] == jnp.mod(me + step, points), shift_id[0], 0))

    row_shift, half_shift = role_shift(row), role_shift(points // 2)
    sent = jnp.stack([row_shift, half_shift])
    lower = lax.ppermute(sent, "ka", to_upper)
    upper = lax.ppermute(sent, "ka", to_lower)
    shifts = jnp.stack([role_shift(1), jnp.where(even, row_shift, lower[0]), lower[1], upper[1]])

    picks = shifts[:, None] == jnp.arange(block_map.shape[0], dtype=jnp.int32)[None, :]
    relabel = jnp.sum(jnp.where(picks[:, :, None], block_map[None], 0), axis=1)
    by_slice = relabel.reshape(relabel.shape[0], 2, slab)
    first = mine == 0
    here = jnp.where(first, by_slice[:, 0], by_slice[:, 1])
    there = jnp.where(first, by_slice[:, 1], by_slice[:, 0])
    crosses_here = (here // slab) != mine
    crosses_there = (there // slab) == mine
    rank_here = jnp.cumsum(crosses_here.astype(jnp.int32), axis=1) - 1
    rank_there = jnp.cumsum(crosses_there.astype(jnp.int32), axis=1) - 1
    places = jnp.arange(capacity, dtype=jnp.int32)
    match_here = crosses_here[:, None, :] & (rank_here[:, None, :] == places[None, :, None])
    match_there = crosses_there[:, None, :] & (rank_there[:, None, :] == places[None, :, None])
    lanes = jnp.arange(slab, dtype=jnp.int32)
    bra_sent = jnp.sum(jnp.where(match_here, lanes[None, None, :], 0), axis=2)
    ket_sent = jnp.sum(jnp.where(match_there, (there - mine * slab)[:, None, :], 0), axis=2)
    ket_at = jnp.sum(jnp.where(match_here, ket_sent[:, :, None], 0), axis=1)
    sends_bra = jnp.stack([even | True, even, even | True, even & False])
    send = jnp.where(sends_bra[:, None], bra_sent, ket_sent)

    up_base, low_base, next_base, around_base, got_base = (slab * n for n in (1, 2, 3, 4, 5))
    bra_base = jnp.stack([0, jnp.where(even, 0, low_base), low_base, up_base])
    ket_base = jnp.stack(
        [jnp.where(column == row - 1, around_base, next_base), jnp.where(even, up_base, 0), up_base, low_base]
    )
    got = got_base + capacity * jnp.arange(4, dtype=jnp.int32)[:, None] + rank_here
    bra_home = bra_base[:, None] + lanes[None, :]
    ket_home = ket_base[:, None] + here - mine * slab
    left = jnp.where(crosses_here & sends_bra[:, None], got, bra_home)
    right = jnp.where(
        crosses_here, jnp.where(sends_bra[:, None], ket_base[:, None] + ket_at, got), ket_home
    )

    size = slab // CHUNKS
    upper_parts = [lax.ppermute(own[c * size : (c + 1) * size], "ka", down) for c in range(CHUNKS)]
    lower_part = lax.ppermute(own, "ka", up)
    next_part = lax.ppermute(own, "ka", direct)
    around_parts = [lax.ppermute(part, "ka", around) for part in upper_parts]
    got_own = lax.ppermute(gather_blocks(send[:2].reshape(-1), own), "ga", swap)
    got_lower = lax.ppermute(gather_blocks(send[2:].reshape(-1), lower_part), "ga", swap)
    sums = dot_items(
        left, right, [own, *upper_parts, lower_part, next_part, *around_parts, got_own, got_lower]
    )

    half = sums.shape[2] // 2
    low_rows, high_rows = sums[:, :, :half], sums[:, :, half:]
    kept = jnp.where(first, low_rows, high_rows)
    total = kept + lax.ppermute(jnp.where(first, high_rows, low_rows), "ga", swap)
    from_upper = lax.ppermute(total[1:3], "ka", to_lower)
    from_lower = lax.ppermute(total[3], "ka", to_upper)
    row_sum = jnp.where(even, total[1], from_upper[0])
    half_sum = from_upper[1] + from_lower
    target = neighbour[0][:, None, None, None]
    out = jnp.where(
        target == jnp.mod(me + 1, points),
        total[0],
        jnp.where(target == jnp.mod(me + row, points), row_sum, half_sum),
    )
    return out[None]


def solution(mesh):
    in_specs = (P("ka", "ga", None, None, None), P("ka", None), P("ka", None), P())
    out_specs = P("ka", None, None, "ga", None)
    four_rows = mesh.shape["ga"] == 2 and mesh.shape["ka"] == 4 * min(16, mesh.shape["ka"] // 4)

    def run(coeffs, neighbour, shift_id, block_map):
        one_each = coeffs.shape[0] == mesh.shape["ka"]
        per_slice = coeffs.shape[1] // mesh.shape["ga"]
        whole_chunks = per_slice % (2 * CHUNKS) == 0 or per_slice % CHUNKS == 0 and per_slice % 2 == 0
        body = on_four_rows if four_rows and one_each and whole_chunks else on_device
        return jax.shard_map(
            body, mesh=mesh, in_specs=in_specs, out_specs=out_specs, check_vma=False
        )(coeffs, neighbour, shift_id, block_map)

    return run
```

```python
import functools

import jax
import jax.numpy as jnp
from jax import lax
from jax.sharding import PartitionSpec as P
from jax.experimental import pallas as pl
from jax.experimental.pallas import tpu as pltpu

CHUNKS = 4


def shifted(block, axis, distance):
    devices = range(lax.axis_size(axis))
    route = [((i - distance) % len(devices), i) for i in devices]
    return lax.ppermute(block, axis, route)


def complex_intersection(bra_real, bra_imag, ket_real, ket_imag, form):
    real_part = jnp.einsum(form, bra_real, ket_real, preferred_element_type=jnp.float32)
    real_part = real_part + jnp.einsum(form, bra_imag, ket_imag, preferred_element_type=jnp.float32)
    imag_part = jnp.einsum(form, bra_real, ket_imag, preferred_element_type=jnp.float32)
    imag_part = imag_part - jnp.einsum(form, bra_imag, ket_real, preferred_element_type=jnp.float32)
    return jnp.stack([real_part, imag_part], axis=-3)


def slot_plan(
    home_slice, target_slice, sent_local, place_local, my_slice, slices, capacity, slab_blocks
):
    targets = jnp.arange(slices, dtype=jnp.int32)
    chosen = (home_slice == my_slice)[:, None, :] & (
        target_slice[:, None, :] == targets[None, :, None]
    )
    chosen = chosen & (targets != my_slice)[None, :, None]
    counted = jnp.cumsum(chosen.astype(jnp.int32), axis=2) - 1
    places = jnp.arange(capacity, dtype=jnp.int32)
    matched = (
        chosen[:, :, None, :] & (counted[:, :, None, :] == places[None, None, :, None])
    ).astype(jnp.int32)
    filled = jnp.sum(matched, axis=3)
    sent_block = jnp.sum(matched * sent_local[:, None, None, :], axis=3)
    where_to = jnp.sum(matched * place_local[:, None, None, :], axis=3) + (1 - filled) * slab_blocks
    pair_count = home_slice.shape[0]
    return (
        sent_block.reshape(pair_count, slices * capacity),
        where_to.reshape(pair_count, slices * capacity),
    )


def on_device(coeffs, neighbour, shift_id, block_map):
    k_local = coeffs.shape[0]
    slab_blocks = coeffs.shape[1]
    band_count = coeffs.shape[3]
    lane_width = coeffs.shape[4]
    vector_count = neighbour.shape[1]
    cycle_size = lax.axis_size("ka")
    slices = lax.axis_size("ga")
    my_cycle = lax.axis_index("ka")
    my_slice = lax.axis_index("ga")
    capacity = 2 * max(1, slab_blocks // 12)
    all_blocks = slab_blocks * slices
    pair_count = k_local * vector_count
    k_total = k_local * cycle_size
    row_points = min(16, k_total // 4)
    row_devices = row_points // k_local
    pad_spec = ((0, 0), (0, 1), (0, 0), (0, 0), (0, 0))
    row_point = shifted(coeffs, "ka", -1)
    row_source = jnp.mod(my_cycle + 1, cycle_size)
    plane_kets = shifted(coeffs, "ka", -row_devices)
    plane_source = jnp.mod(my_cycle + row_devices, cycle_size)
    opposite = shifted(coeffs, "ka", cycle_size // 2)
    targets_flat = neighbour.reshape(-1)
    shifts_flat = shift_id.reshape(-1)
    target_device = targets_flat // k_local
    target_lane = targets_flat - target_device * k_local
    ket_index = jnp.where(
        target_device == my_cycle,
        target_lane,
        jnp.where(
            target_device == row_source,
            k_local,
            jnp.where(
                target_device == plane_source,
                k_local + 1 + target_lane,
                2 * k_local + 1 + target_lane,
            ),
        ),
    )
    bra_index = jnp.arange(pair_count, dtype=jnp.int32) // vector_count
    picks = (
        shifts_flat[:, None] == jnp.arange(block_map.shape[0], dtype=jnp.int32)[None, :]
    ).astype(jnp.int32)
    relabel = jnp.sum(picks[:, :, None] * block_map[None, :, :], axis=1)
    dest_global = jnp.broadcast_to(jnp.arange(all_blocks, dtype=jnp.int32)[None, :], relabel.shape)
    source_slice = relabel // slab_blocks
    dest_slice = dest_global // slab_blocks
    source_local = relabel - source_slice * slab_blocks
    dest_local = dest_global - dest_slice * slab_blocks
    kets = jnp.pad(jnp.concatenate([coeffs, row_point, plane_kets, opposite], axis=0), pad_spec)
    own_source = lax.dynamic_slice_in_dim(relabel, my_slice * slab_blocks, slab_blocks, 1)
    self_place = jnp.where(
        own_source // slab_blocks == my_slice, own_source - my_slice * slab_blocks, slab_blocks
    )
    ket_self = kets[ket_index[:, None], self_place]
    ket_self = ket_self.reshape(k_local, vector_count, slab_blocks, 2, band_count, lane_width)
    local_terms = complex_intersection(
        coeffs[:, :, 0],
        coeffs[:, :, 1],
        ket_self[:, :, :, 0],
        ket_self[:, :, :, 1],
        "ksmw,kbsnw->kbmn",
    )
    sent_block, where_to = slot_plan(
        dest_slice, source_slice, dest_local, source_local, my_slice, slices, capacity, slab_blocks
    )
    payload = coeffs[bra_index[:, None], sent_block]
    owner = jnp.broadcast_to(ket_index[:, None], (pair_count, slices))
    blocks = lax.all_to_all(payload, "ga", split_axis=1, concat_axis=1, tiled=True)
    places_in = lax.all_to_all(where_to, "ga", split_axis=1, concat_axis=1, tiled=True)
    owners = lax.all_to_all(owner, "ga", split_axis=1, concat_axis=1, tiled=True)
    partner = kets[owners[:, 0][:, None], places_in]
    remote = complex_intersection(
        blocks[:, :, 0], blocks[:, :, 1], partner[:, :, 0], partner[:, :, 1], "ismw,isnw->imn"
    )
    summed_part = local_terms + remote.reshape(k_local, vector_count, 2, band_count, band_count)
    total = lax.psum(summed_part, "ga")
    row_count = band_count // slices
    return lax.dynamic_slice_in_dim(total, my_slice * row_count, row_count, 3)


def gather_kernel(count, index_ref, source_ref, out_ref, sems):
    def copy(i):
        return pltpu.make_async_copy(source_ref.at[index_ref[i]], out_ref.at[i], sems.at[i])

    def begin(i, carry):
        copy(i).start()
        return carry

    def finish(i, carry):
        copy(i).wait()
        return carry

    lax.fori_loop(0, count, begin, 0)
    lax.fori_loop(0, count, finish, 0)


def gather_blocks(index, source):
    count = index.shape[0]
    shape = (count,) + source.shape[1:]
    return pl.pallas_call(
        functools.partial(gather_kernel, count),
        out_shape=jax.ShapeDtypeStruct(shape, source.dtype),
        in_specs=[
            pl.BlockSpec(memory_space=pltpu.SMEM),
            pl.BlockSpec(memory_space=pl.ANY),
        ],
        out_specs=pl.BlockSpec(memory_space=pltpu.VMEM),
        scratch_shapes=[pltpu.SemaphoreType.DMA((count,))],
        name="gather_blocks",
        cost_estimate=pl.CostEstimate(flops=0, bytes_accessed=4 * source.dtype.itemsize * count * source[0].size, transcendentals=0),
    )(index, source)


def plan_kernel(slab, capacity, shift_ref, map_ref, local_ref, sent_ref, got_ref):
    mine = lax.axis_index("ga")
    base = mine * slab
    for e in range(4):
        shift = shift_ref[e]

        def here(j, counts):
            own, out = counts
            source = map_ref[shift, base + j] - base
            inside = (source >= 0) & (source < slab)
            local_ref[0, e, own] = j
            local_ref[1, e, own] = source
            sent_ref[e, out] = j
            return own + inside.astype(jnp.int32), out + 1 - inside.astype(jnp.int32)

        def there(j, count):
            source = map_ref[shift, slab - base + j] - base
            inside = (source >= 0) & (source < slab)
            got_ref[e, count] = source
            return count + inside.astype(jnp.int32)

        lax.fori_loop(0, slab, here, (jnp.int32(0), jnp.int32(0)), unroll=8)
        lax.fori_loop(0, slab, there, jnp.int32(0), unroll=8)


def plan(shifts, block_map, slab, capacity):
    own_count = slab - capacity
    return pl.pallas_call(
        functools.partial(plan_kernel, slab, capacity),
        out_shape=(
            jax.ShapeDtypeStruct((2, 4, own_count + 8), jnp.int32),
            jax.ShapeDtypeStruct((4, capacity + 8), jnp.int32),
            jax.ShapeDtypeStruct((4, capacity + 8), jnp.int32),
        ),
        in_specs=[pl.BlockSpec(memory_space=pltpu.SMEM)] * 2,
        out_specs=[pl.BlockSpec(memory_space=pltpu.SMEM)] * 3,
        name="plan",
    )(shifts, block_map)


def meet_kernel(
    points, slab, capacity, local_ref, other_ref, send_ref, own_hbm, mine_out, out_ref,
    own, upper, lower, nxt, got_own, lower_out, got_lower, local_sems, send_sems, recv_sems,
):
    row = points // 4
    me = lax.axis_index("ka")
    partner = 1 - lax.axis_index("ga")
    z, column = me // row, me % row
    even = column % 2 == 0
    middle = (z == 1) | (z == 2)
    holds_pair = (even & ~middle) | (~even & middle)
    below = {"ka": (me + points - row) % points}
    above = {"ka": (me + row) % points}
    left = {"ka": z * row + (column + row - 1) % row}
    right = {"ka": z * row + (column + 1) % row}
    across = {"ga": partner}
    bands, lanes = own.shape[2], own.shape[3]
    size = slab // CHUNKS
    own_count = slab - capacity

    barrier = pltpu.get_barrier_semaphore()
    for peer in (below, above, left, right, across):
        pl.semaphore_signal(barrier, inc=1, device_id=peer, device_id_type=pl.DeviceIdType.MESH)
    pl.semaphore_wait(barrier, 5)

    def remote(source, target, n, peer):
        return pltpu.make_async_remote_copy(
            src_ref=source, dst_ref=target, send_sem=send_sems.at[n], recv_sem=recv_sems.at[n],
            device_id=peer, device_id_type=pl.DeviceIdType.MESH,
        )

    def chunk(c):
        return pl.ds(c * size, size)

    keep = pltpu.make_async_copy(own_hbm, own, local_sems.at[0])
    swap_own = remote(mine_out, got_own, 0, across)
    swap_lower = remote(lower_out, got_lower, 1, across)
    rise = [remote(own_hbm.at[chunk(c)], lower.at[chunk(c)], 2 + c, above) for c in range(CHUNKS)]
    fall = [remote(own_hbm.at[chunk(c)], upper.at[chunk(c)], 2 + CHUNKS + c, below) for c in range(CHUNKS)]
    pass_own = [remote(own_hbm.at[chunk(c)], nxt.at[chunk(c)], 2 + 2 * CHUNKS + c, left) for c in range(CHUNKS)]
    pass_on = [remote(upper.at[chunk(c)], nxt.at[chunk(c)], 2 + 2 * CHUNKS + c, left) for c in range(CHUNKS)]

    falls = even | (z >= 2)
    rises = ~even | (z >= 2)
    gets_upper = even | middle
    gets_lower = ~even | ~middle

    @pl.when(falls)
    def _():
        for copy in fall:
            copy.start()

    @pl.when(rises)
    def _():
        for copy in rise:
            copy.start()

    @pl.when(column > 0)
    def _():
        for copy in pass_own:
            copy.start()

    swap_own.start()
    keep.start()

    def pick(ref, at):
        return ref[at].reshape(2 * bands, lanes)

    def product(total, first_left, second_left, first_right, second_right):
        return total + lax.dot_general(
            jnp.concatenate([first_left, second_left], axis=1),
            jnp.concatenate([first_right, second_right], axis=1),
            (((1,), (1,)), ((), ())),
            preferred_element_type=jnp.float32,
        )

    def edge(e, bra, ket, got, got_at, bra_sent):
        def own_step(i, total):
            for u in range(0, 10, 2):
                n = i * 10 + u
                total = product(
                    total,
                    pick(bra, local_ref[0, e, n]), pick(bra, local_ref[0, e, n + 1]),
                    pick(ket, local_ref[1, e, n]), pick(ket, local_ref[1, e, n + 1]),
                )
            return total

        def cross_step(i, total):
            n = i * 2
            travelled = pick(got, got_at + n), pick(got, got_at + n + 1)
            stayed_ref = ket if bra_sent else bra
            stayed = pick(stayed_ref, other_ref[e, n]), pick(stayed_ref, other_ref[e, n + 1])
            if bra_sent:
                return product(total, *travelled, *stayed)
            return product(total, *stayed, *travelled)

        total = jnp.zeros((2 * bands, 2 * bands), jnp.float32)
        total = lax.fori_loop(0, own_count // 10, own_step, total)
        total = lax.fori_loop(0, capacity // 2, cross_step, total)
        out_ref[e, 0] = total[:bands, :bands] + total[bands:, bands:]
        out_ref[e, 1] = total[:bands, bands:] - total[bands:, :bands]

    keep.wait()
    swap_own.wait_recv()

    def next_edge():
        for copy in pass_own:
            copy.wait_recv()
        edge(0, own, nxt, got_own, 0, True)

    @pl.when(column < row - 1)
    def _():
        next_edge()

    @pl.when(gets_upper)
    def _():
        for copy, onward in zip(fall, pass_on):
            copy.wait_recv()

            @pl.when(column == 0)
            def _():
                onward.start()

    @pl.when(gets_lower)
    def _():
        for copy in rise:
            copy.wait_recv()

    @pl.when(holds_pair)
    def _():
        def gather(r, carry):
            lower_out[r] = lower[send_ref[r]]
            return carry

        lax.fori_loop(0, 2 * capacity, gather, 0)
        swap_lower.start()

    @pl.when(even)
    def _():
        edge(1, own, upper, got_own, capacity, True)

    @pl.when(~even)
    def _():
        edge(1, lower, own, got_own, capacity, False)

    @pl.when(column == row - 1)
    def _():
        next_edge()

    @pl.when(holds_pair)
    def _():
        swap_lower.wait_recv()
        edge(2, lower, upper, got_lower, 0, True)
        edge(3, upper, lower, got_lower, capacity, False)
        swap_lower.wait_send()

    @pl.when(~holds_pair)
    def _():
        out_ref[2] = jnp.zeros_like(out_ref[2])
        out_ref[3] = jnp.zeros_like(out_ref[3])

    swap_own.wait_send()

    @pl.when(falls)
    def _():
        for copy in fall:
            copy.wait_send()

    @pl.when(rises)
    def _():
        for copy in rise:
            copy.wait_send()

    @pl.when(column > 0)
    def _():
        for copy in pass_own:
            copy.wait_send()

    @pl.when(column == 0)
    def _():
        for copy in pass_on:
            copy.wait_send()


def meet(local, other, send, own, mine_out, points, capacity):
    slab, bands = own.shape[0], own.shape[2]
    block = own.shape[1:]
    copies = 2 + 3 * CHUNKS
    return pl.pallas_call(
        functools.partial(meet_kernel, points, slab, capacity),
        out_shape=jax.ShapeDtypeStruct((4, 2, bands, bands), jnp.float32),
        in_specs=[pl.BlockSpec(memory_space=pltpu.SMEM)] * 3 + [pl.BlockSpec(memory_space=pl.ANY)] * 2,
        out_specs=pl.BlockSpec(memory_space=pltpu.VMEM),
        scratch_shapes=[pltpu.VMEM((slab,) + block, own.dtype)] * 4
        + [pltpu.VMEM((2 * capacity,) + block, own.dtype)] * 3
        + [pltpu.SemaphoreType.DMA((1,)), pltpu.SemaphoreType.DMA((copies,)), pltpu.SemaphoreType.DMA((copies,))],
        compiler_params=pltpu.CompilerParams(
            collective_id=0, has_side_effects=True, vmem_limit_bytes=32 * 2**20
        ),
        name="meet",
    )(local, other, send, own, mine_out)


def on_four_rows(coeffs, neighbour, shift_id, block_map):
    own = coeffs[0]
    slab = own.shape[0]
    points = lax.axis_size("ka")
    row = points // 4
    me = lax.axis_index("ka")
    first = lax.axis_index("ga") == 0
    even = jnp.mod(jnp.mod(me, row), 2) == 0
    capacity = 2 * max(1, slab // 12)
    to_lower = [((k + row) % points, k) for k in range(points)]
    to_upper = [((k - row) % points, k) for k in range(points)]
    swap = [(0, 1), (1, 0)]

    def role_shift(step):
        return jnp.sum(jnp.where(neighbour[0] == jnp.mod(me + step, points), shift_id[0], 0))

    row_shift, half_shift = role_shift(row), role_shift(points // 2)
    sent = jnp.stack([row_shift, half_shift])
    lower = lax.ppermute(sent, "ka", to_upper)
    upper = lax.ppermute(sent, "ka", to_lower)
    shifts = jnp.stack([role_shift(1), jnp.where(even, row_shift, lower[0]), lower[1], upper[1]])

    local, bras, kets = plan(shifts, block_map, slab, capacity)
    bras, kets = bras[:, :capacity], kets[:, :capacity]
    sends_bra = jnp.stack([even | True, even, even | True, even & False])[:, None]
    send = jnp.where(sends_bra, bras, kets)
    other = jnp.where(sends_bra, kets, bras)
    mine_out = gather_blocks(send[:2].reshape(-1), own)
    sums = meet(local, other, send[2:].reshape(-1), own, mine_out, points, capacity)

    half = sums.shape[2] // 2
    low_rows, high_rows = sums[:, :, :half], sums[:, :, half:]
    kept = jnp.where(first, low_rows, high_rows)
    total = kept + lax.ppermute(jnp.where(first, high_rows, low_rows), "ga", swap)
    from_upper = lax.ppermute(total[1:3], "ka", to_lower)
    from_lower = lax.ppermute(total[3], "ka", to_upper)
    row_sum = jnp.where(even, total[1], from_upper[0])
    half_sum = from_upper[1] + from_lower
    target = neighbour[0][:, None, None, None]
    out = jnp.where(
        target == jnp.mod(me + 1, points),
        total[0],
        jnp.where(target == jnp.mod(me + row, points), row_sum, half_sum),
    )
    return out[None]


def solution(mesh):
    in_specs = (P("ka", "ga", None, None, None), P("ka", None), P("ka", None), P())
    out_specs = P("ka", None, None, "ga", None)
    four_rows = mesh.shape["ga"] == 2 and mesh.shape["ka"] == 4 * min(16, mesh.shape["ka"] // 4)

    def run(coeffs, neighbour, shift_id, block_map):
        one_each = coeffs.shape[0] == mesh.shape["ka"]
        per_slice = coeffs.shape[1] // mesh.shape["ga"]
        whole_chunks = per_slice % (2 * CHUNKS) == 0 or per_slice % CHUNKS == 0 and per_slice % 2 == 0
        body = on_four_rows if four_rows and one_each and whole_chunks else on_device
        return jax.shard_map(
            body, mesh=mesh, in_specs=in_specs, out_specs=out_specs, check_vma=False
        )(coeffs, neighbour, shift_id, block_map)

    return run
```

```python
import functools

import jax
import jax.numpy as jnp
from jax import lax
from jax.sharding import PartitionSpec as P
from jax.experimental import pallas as pl
from jax.experimental.pallas import tpu as pltpu

CHUNKS = 4


def shifted(block, axis, distance):
    devices = range(lax.axis_size(axis))
    route = [((i - distance) % len(devices), i) for i in devices]
    return lax.ppermute(block, axis, route)


def complex_intersection(bra_real, bra_imag, ket_real, ket_imag, form):
    real_part = jnp.einsum(form, bra_real, ket_real, preferred_element_type=jnp.float32)
    real_part = real_part + jnp.einsum(form, bra_imag, ket_imag, preferred_element_type=jnp.float32)
    imag_part = jnp.einsum(form, bra_real, ket_imag, preferred_element_type=jnp.float32)
    imag_part = imag_part - jnp.einsum(form, bra_imag, ket_real, preferred_element_type=jnp.float32)
    return jnp.stack([real_part, imag_part], axis=-3)


def slot_plan(
    home_slice, target_slice, sent_local, place_local, my_slice, slices, capacity, slab_blocks
):
    targets = jnp.arange(slices, dtype=jnp.int32)
    chosen = (home_slice == my_slice)[:, None, :] & (
        target_slice[:, None, :] == targets[None, :, None]
    )
    chosen = chosen & (targets != my_slice)[None, :, None]
    counted = jnp.cumsum(chosen.astype(jnp.int32), axis=2) - 1
    places = jnp.arange(capacity, dtype=jnp.int32)
    matched = (
        chosen[:, :, None, :] & (counted[:, :, None, :] == places[None, None, :, None])
    ).astype(jnp.int32)
    filled = jnp.sum(matched, axis=3)
    sent_block = jnp.sum(matched * sent_local[:, None, None, :], axis=3)
    where_to = jnp.sum(matched * place_local[:, None, None, :], axis=3) + (1 - filled) * slab_blocks
    pair_count = home_slice.shape[0]
    return (
        sent_block.reshape(pair_count, slices * capacity),
        where_to.reshape(pair_count, slices * capacity),
    )


def on_device(coeffs, neighbour, shift_id, block_map):
    k_local = coeffs.shape[0]
    slab_blocks = coeffs.shape[1]
    band_count = coeffs.shape[3]
    lane_width = coeffs.shape[4]
    vector_count = neighbour.shape[1]
    cycle_size = lax.axis_size("ka")
    slices = lax.axis_size("ga")
    my_cycle = lax.axis_index("ka")
    my_slice = lax.axis_index("ga")
    capacity = 2 * max(1, slab_blocks // 12)
    all_blocks = slab_blocks * slices
    pair_count = k_local * vector_count
    k_total = k_local * cycle_size
    row_points = min(16, k_total // 4)
    row_devices = row_points // k_local
    pad_spec = ((0, 0), (0, 1), (0, 0), (0, 0), (0, 0))
    row_point = shifted(coeffs, "ka", -1)
    row_source = jnp.mod(my_cycle + 1, cycle_size)
    plane_kets = shifted(coeffs, "ka", -row_devices)
    plane_source = jnp.mod(my_cycle + row_devices, cycle_size)
    opposite = shifted(coeffs, "ka", cycle_size // 2)
    targets_flat = neighbour.reshape(-1)
    shifts_flat = shift_id.reshape(-1)
    target_device = targets_flat // k_local
    target_lane = targets_flat - target_device * k_local
    ket_index = jnp.where(
        target_device == my_cycle,
        target_lane,
        jnp.where(
            target_device == row_source,
            k_local,
            jnp.where(
                target_device == plane_source,
                k_local + 1 + target_lane,
                2 * k_local + 1 + target_lane,
            ),
        ),
    )
    bra_index = jnp.arange(pair_count, dtype=jnp.int32) // vector_count
    picks = (
        shifts_flat[:, None] == jnp.arange(block_map.shape[0], dtype=jnp.int32)[None, :]
    ).astype(jnp.int32)
    relabel = jnp.sum(picks[:, :, None] * block_map[None, :, :], axis=1)
    dest_global = jnp.broadcast_to(jnp.arange(all_blocks, dtype=jnp.int32)[None, :], relabel.shape)
    source_slice = relabel // slab_blocks
    dest_slice = dest_global // slab_blocks
    source_local = relabel - source_slice * slab_blocks
    dest_local = dest_global - dest_slice * slab_blocks
    kets = jnp.pad(jnp.concatenate([coeffs, row_point, plane_kets, opposite], axis=0), pad_spec)
    own_source = lax.dynamic_slice_in_dim(relabel, my_slice * slab_blocks, slab_blocks, 1)
    self_place = jnp.where(
        own_source // slab_blocks == my_slice, own_source - my_slice * slab_blocks, slab_blocks
    )
    ket_self = kets[ket_index[:, None], self_place]
    ket_self = ket_self.reshape(k_local, vector_count, slab_blocks, 2, band_count, lane_width)
    local_terms = complex_intersection(
        coeffs[:, :, 0],
        coeffs[:, :, 1],
        ket_self[:, :, :, 0],
        ket_self[:, :, :, 1],
        "ksmw,kbsnw->kbmn",
    )
    sent_block, where_to = slot_plan(
        dest_slice, source_slice, dest_local, source_local, my_slice, slices, capacity, slab_blocks
    )
    payload = coeffs[bra_index[:, None], sent_block]
    owner = jnp.broadcast_to(ket_index[:, None], (pair_count, slices))
    blocks = lax.all_to_all(payload, "ga", split_axis=1, concat_axis=1, tiled=True)
    places_in = lax.all_to_all(where_to, "ga", split_axis=1, concat_axis=1, tiled=True)
    owners = lax.all_to_all(owner, "ga", split_axis=1, concat_axis=1, tiled=True)
    partner = kets[owners[:, 0][:, None], places_in]
    remote = complex_intersection(
        blocks[:, :, 0], blocks[:, :, 1], partner[:, :, 0], partner[:, :, 1], "ismw,isnw->imn"
    )
    summed_part = local_terms + remote.reshape(k_local, vector_count, 2, band_count, band_count)
    total = lax.psum(summed_part, "ga")
    row_count = band_count // slices
    return lax.dynamic_slice_in_dim(total, my_slice * row_count, row_count, 3)


def gather_kernel(count, index_ref, source_ref, out_ref, sems):
    def copy(i):
        return pltpu.make_async_copy(source_ref.at[index_ref[i]], out_ref.at[i], sems.at[i])

    def begin(i, carry):
        copy(i).start()
        return carry

    def finish(i, carry):
        copy(i).wait()
        return carry

    lax.fori_loop(0, count, begin, 0)
    lax.fori_loop(0, count, finish, 0)


def gather_blocks(index, source):
    count = index.shape[0]
    shape = (count,) + source.shape[1:]
    return pl.pallas_call(
        functools.partial(gather_kernel, count),
        out_shape=jax.ShapeDtypeStruct(shape, source.dtype),
        in_specs=[
            pl.BlockSpec(memory_space=pltpu.SMEM),
            pl.BlockSpec(memory_space=pl.ANY),
        ],
        out_specs=pl.BlockSpec(memory_space=pltpu.VMEM),
        scratch_shapes=[pltpu.SemaphoreType.DMA((count,))],
        name="gather_blocks",
        cost_estimate=pl.CostEstimate(flops=0, bytes_accessed=4 * source.dtype.itemsize * count * source[0].size, transcendentals=0),
    )(index, source)


def plan_kernel(slab, capacity, shift_ref, map_ref, local_ref, sent_ref, got_ref):
    mine = lax.axis_index("ga")
    base = mine * slab
    for e in range(4):
        shift = shift_ref[e]

        def here(j, counts):
            own, out = counts
            source = map_ref[shift, base + j] - base
            inside = (source >= 0) & (source < slab)
            local_ref[0, e, own] = j
            local_ref[1, e, own] = source
            sent_ref[e, out] = j
            return own + inside.astype(jnp.int32), out + 1 - inside.astype(jnp.int32)

        def there(j, count):
            source = map_ref[shift, slab - base + j] - base
            inside = (source >= 0) & (source < slab)
            got_ref[e, count] = source
            return count + inside.astype(jnp.int32)

        lax.fori_loop(0, slab, here, (jnp.int32(0), jnp.int32(0)), unroll=8)
        lax.fori_loop(0, slab, there, jnp.int32(0), unroll=8)


def plan(shifts, block_map, slab, capacity):
    own_count = slab - capacity
    return pl.pallas_call(
        functools.partial(plan_kernel, slab, capacity),
        out_shape=(
            jax.ShapeDtypeStruct((2, 4, own_count + 8), jnp.int32),
            jax.ShapeDtypeStruct((4, capacity + 8), jnp.int32),
            jax.ShapeDtypeStruct((4, capacity + 8), jnp.int32),
        ),
        in_specs=[pl.BlockSpec(memory_space=pltpu.SMEM)] * 2,
        out_specs=[pl.BlockSpec(memory_space=pltpu.SMEM)] * 3,
        name="plan",
    )(shifts, block_map)


def meet_kernel(
    points, slab, capacity, local_ref, other_ref, send_ref, own_hbm, mine_out, out_ref,
    own, upper, lower, nxt, got_own, lower_out, got_lower, local_sems, send_sems, recv_sems,
):
    row = points // 4
    me = lax.axis_index("ka")
    partner = 1 - lax.axis_index("ga")
    z, column = me // row, me % row
    even = column % 2 == 0
    middle = (z == 1) | (z == 2)
    holds_pair = middle
    below = {"ka": (me + points - row) % points}
    above = {"ka": (me + row) % points}
    left = {"ka": z * row + (column + row - 1) % row}
    right = {"ka": z * row + (column + 1) % row}
    across = {"ga": partner}
    bands, lanes = own.shape[2], own.shape[3]
    size = slab // CHUNKS
    own_count = slab - capacity

    barrier = pltpu.get_barrier_semaphore()
    for peer in (below, above, left, right, across):
        pl.semaphore_signal(barrier, inc=1, device_id=peer, device_id_type=pl.DeviceIdType.MESH)
    pl.semaphore_wait(barrier, 5)

    def remote(source, target, n, peer):
        return pltpu.make_async_remote_copy(
            src_ref=source, dst_ref=target, send_sem=send_sems.at[n], recv_sem=recv_sems.at[n],
            device_id=peer, device_id_type=pl.DeviceIdType.MESH,
        )

    def chunk(c):
        return pl.ds(c * size, size)

    keep = pltpu.make_async_copy(own_hbm, own, local_sems.at[0])
    swap_own = remote(mine_out, got_own, 0, across)
    swap_lower = remote(lower_out, got_lower, 1, across)
    rise = [remote(own_hbm.at[chunk(c)], lower.at[chunk(c)], 2 + c, above) for c in range(CHUNKS)]
    fall = [remote(own_hbm.at[chunk(c)], upper.at[chunk(c)], 2 + CHUNKS + c, below) for c in range(CHUNKS)]
    pass_own = [remote(own_hbm.at[chunk(c)], nxt.at[chunk(c)], 2 + 2 * CHUNKS + c, left) for c in range(CHUNKS)]
    pass_on = [remote(upper.at[chunk(c)], nxt.at[chunk(c)], 2 + 2 * CHUNKS + c, left) for c in range(CHUNKS)]

    falls = even | (z >= 2)
    rises = ~even | (z <= 1)
    gets_upper = even | middle
    gets_lower = ~even | middle

    keep.start()
    swap_own.start()
    for c in range(CHUNKS):

        @pl.when(column > 0)
        def _():
            pass_own[c].start()

        @pl.when(falls)
        def _():
            fall[c].start()

        @pl.when(rises)
        def _():
            rise[c].start()

    def pick(ref, at):
        return ref[at].reshape(2 * bands, lanes)

    def product(total, first_left, second_left, first_right, second_right):
        return total + lax.dot_general(
            jnp.concatenate([first_left, second_left], axis=1),
            jnp.concatenate([first_right, second_right], axis=1),
            (((1,), (1,)), ((), ())),
            preferred_element_type=jnp.float32,
        )

    def edge(e, bra, ket, got, got_at, bra_sent):
        def own_step(i, total):
            for u in range(0, 10, 2):
                n = i * 10 + u
                total = product(
                    total,
                    pick(bra, local_ref[0, e, n]), pick(bra, local_ref[0, e, n + 1]),
                    pick(ket, local_ref[1, e, n]), pick(ket, local_ref[1, e, n + 1]),
                )
            return total

        def cross_step(i, total):
            n = i * 2
            travelled = pick(got, got_at + n), pick(got, got_at + n + 1)
            stayed_ref = ket if bra_sent else bra
            stayed = pick(stayed_ref, other_ref[e, n]), pick(stayed_ref, other_ref[e, n + 1])
            if bra_sent:
                return product(total, *travelled, *stayed)
            return product(total, *stayed, *travelled)

        total = jnp.zeros((2 * bands, 2 * bands), jnp.float32)
        total = lax.fori_loop(0, own_count // 10, own_step, total)
        total = lax.fori_loop(0, capacity // 2, cross_step, total)
        out_ref[e, 0] = total[:bands, :bands] + total[bands:, bands:]
        out_ref[e, 1] = total[:bands, bands:] - total[bands:, :bands]

    keep.wait()
    swap_own.wait_recv()

    def next_edge():
        for copy in pass_own:
            copy.wait_recv()
        edge(0, own, nxt, got_own, 0, True)

    @pl.when(column < row - 1)
    def _():
        next_edge()

    @pl.when(gets_upper)
    def _():
        for copy, onward in zip(fall, pass_on):
            copy.wait_recv()

            @pl.when(column == 0)
            def _():
                onward.start()

    @pl.when(gets_lower)
    def _():
        for copy in rise:
            copy.wait_recv()

    @pl.when(holds_pair)
    def _():
        def gather(r, carry):
            lower_out[r] = lower[send_ref[r]]
            return carry

        lax.fori_loop(0, 2 * capacity, gather, 0)
        swap_lower.start()

    @pl.when(even)
    def _():
        edge(1, own, upper, got_own, capacity, True)

    @pl.when(~even)
    def _():
        edge(1, lower, own, got_own, capacity, False)

    @pl.when(column == row - 1)
    def _():
        next_edge()

    @pl.when(holds_pair)
    def _():
        swap_lower.wait_recv()
        edge(2, lower, upper, got_lower, 0, True)
        edge(3, upper, lower, got_lower, capacity, False)
        swap_lower.wait_send()

    @pl.when(~holds_pair)
    def _():
        out_ref[2] = jnp.zeros_like(out_ref[2])
        out_ref[3] = jnp.zeros_like(out_ref[3])

    swap_own.wait_send()

    @pl.when(falls)
    def _():
        for copy in fall:
            copy.wait_send()

    @pl.when(rises)
    def _():
        for copy in rise:
            copy.wait_send()

    @pl.when(column > 0)
    def _():
        for copy in pass_own:
            copy.wait_send()

    @pl.when(column == 0)
    def _():
        for copy in pass_on:
            copy.wait_send()


def meet(local, other, send, own, mine_out, points, capacity):
    slab, bands = own.shape[0], own.shape[2]
    block = own.shape[1:]
    copies = 2 + 3 * CHUNKS
    return pl.pallas_call(
        functools.partial(meet_kernel, points, slab, capacity),
        out_shape=jax.ShapeDtypeStruct((4, 2, bands, bands), jnp.float32),
        in_specs=[pl.BlockSpec(memory_space=pltpu.SMEM)] * 3 + [pl.BlockSpec(memory_space=pl.ANY)] * 2,
        out_specs=pl.BlockSpec(memory_space=pltpu.VMEM),
        scratch_shapes=[pltpu.VMEM((slab,) + block, own.dtype)] * 4
        + [pltpu.VMEM((2 * capacity,) + block, own.dtype)] * 3
        + [pltpu.SemaphoreType.DMA((1,)), pltpu.SemaphoreType.DMA((copies,)), pltpu.SemaphoreType.DMA((copies,))],
        compiler_params=pltpu.CompilerParams(
            collective_id=0, has_side_effects=True, vmem_limit_bytes=32 * 2**20
        ),
        name="meet",
    )(local, other, send, own, mine_out)


def on_four_rows(coeffs, neighbour, shift_id, block_map):
    own = coeffs[0]
    slab = own.shape[0]
    points = lax.axis_size("ka")
    row = points // 4
    me = lax.axis_index("ka")
    first = lax.axis_index("ga") == 0
    even = jnp.mod(jnp.mod(me, row), 2) == 0
    capacity = 2 * max(1, slab // 12)
    to_lower = [((k + row) % points, k) for k in range(points)]
    to_upper = [((k - row) % points, k) for k in range(points)]
    swap = [(0, 1), (1, 0)]

    def role_shift(step):
        return jnp.sum(jnp.where(neighbour[0] == jnp.mod(me + step, points), shift_id[0], 0))

    row_shift, half_shift = role_shift(row), role_shift(points // 2)
    sent = jnp.stack([row_shift, half_shift])
    lower = lax.ppermute(sent, "ka", to_upper)
    upper = lax.ppermute(sent, "ka", to_lower)
    shifts = jnp.stack([role_shift(1), jnp.where(even, row_shift, lower[0]), lower[1], upper[1]])

    local, bras, kets = plan(shifts, block_map, slab, capacity)
    bras, kets = bras[:, :capacity], kets[:, :capacity]
    sends_bra = jnp.stack([even | True, even, even | True, even & False])[:, None]
    send = jnp.where(sends_bra, bras, kets)
    other = jnp.where(sends_bra, kets, bras)
    mine_out = gather_blocks(send[:2].reshape(-1), own)
    sums = meet(local, other, send[2:].reshape(-1), own, mine_out, points, capacity)

    half = sums.shape[2] // 2
    low_rows, high_rows = sums[:, :, :half], sums[:, :, half:]
    kept = jnp.where(first, low_rows, high_rows)
    total = kept + lax.ppermute(jnp.where(first, high_rows, low_rows), "ga", swap)
    from_upper = lax.ppermute(total[1:3], "ka", to_lower)
    from_lower = lax.ppermute(total[3], "ka", to_upper)
    row_sum = jnp.where(even, total[1], from_upper[0])
    half_sum = from_upper[1] + from_lower
    target = neighbour[0][:, None, None, None]
    out = jnp.where(
        target == jnp.mod(me + 1, points),
        total[0],
        jnp.where(target == jnp.mod(me + row, points), row_sum, half_sum),
    )
    return out[None]


def solution(mesh):
    in_specs = (P("ka", "ga", None, None, None), P("ka", None), P("ka", None), P())
    out_specs = P("ka", None, None, "ga", None)
    four_rows = mesh.shape["ga"] == 2 and mesh.shape["ka"] == 4 * min(16, mesh.shape["ka"] // 4)

    def run(coeffs, neighbour, shift_id, block_map):
        one_each = coeffs.shape[0] == mesh.shape["ka"]
        per_slice = coeffs.shape[1] // mesh.shape["ga"]
        whole_chunks = per_slice % (2 * CHUNKS) == 0 or per_slice % CHUNKS == 0 and per_slice % 2 == 0
        body = on_four_rows if four_rows and one_each and whole_chunks else on_device
        return jax.shard_map(
            body, mesh=mesh, in_specs=in_specs, out_specs=out_specs, check_vma=False
        )(coeffs, neighbour, shift_id, block_map)

    return run
```

```python
import functools

import jax
import jax.numpy as jnp
from jax import lax
from jax.sharding import PartitionSpec as P
from jax.experimental import pallas as pl
from jax.experimental.pallas import tpu as pltpu

CHUNKS = 4


def shifted(block, axis, distance):
    devices = range(lax.axis_size(axis))
    route = [((i - distance) % len(devices), i) for i in devices]
    return lax.ppermute(block, axis, route)


def complex_intersection(bra_real, bra_imag, ket_real, ket_imag, form):
    real_part = jnp.einsum(form, bra_real, ket_real, preferred_element_type=jnp.float32)
    real_part = real_part + jnp.einsum(form, bra_imag, ket_imag, preferred_element_type=jnp.float32)
    imag_part = jnp.einsum(form, bra_real, ket_imag, preferred_element_type=jnp.float32)
    imag_part = imag_part - jnp.einsum(form, bra_imag, ket_real, preferred_element_type=jnp.float32)
    return jnp.stack([real_part, imag_part], axis=-3)


def slot_plan(
    home_slice, target_slice, sent_local, place_local, my_slice, slices, capacity, slab_blocks
):
    targets = jnp.arange(slices, dtype=jnp.int32)
    chosen = (home_slice == my_slice)[:, None, :] & (
        target_slice[:, None, :] == targets[None, :, None]
    )
    chosen = chosen & (targets != my_slice)[None, :, None]
    counted = jnp.cumsum(chosen.astype(jnp.int32), axis=2) - 1
    places = jnp.arange(capacity, dtype=jnp.int32)
    matched = (
        chosen[:, :, None, :] & (counted[:, :, None, :] == places[None, None, :, None])
    ).astype(jnp.int32)
    filled = jnp.sum(matched, axis=3)
    sent_block = jnp.sum(matched * sent_local[:, None, None, :], axis=3)
    where_to = jnp.sum(matched * place_local[:, None, None, :], axis=3) + (1 - filled) * slab_blocks
    pair_count = home_slice.shape[0]
    return (
        sent_block.reshape(pair_count, slices * capacity),
        where_to.reshape(pair_count, slices * capacity),
    )


def on_device(coeffs, neighbour, shift_id, block_map):
    k_local = coeffs.shape[0]
    slab_blocks = coeffs.shape[1]
    band_count = coeffs.shape[3]
    lane_width = coeffs.shape[4]
    vector_count = neighbour.shape[1]
    cycle_size = lax.axis_size("ka")
    slices = lax.axis_size("ga")
    my_cycle = lax.axis_index("ka")
    my_slice = lax.axis_index("ga")
    capacity = 2 * max(1, slab_blocks // 12)
    all_blocks = slab_blocks * slices
    pair_count = k_local * vector_count
    k_total = k_local * cycle_size
    row_points = min(16, k_total // 4)
    row_devices = row_points // k_local
    pad_spec = ((0, 0), (0, 1), (0, 0), (0, 0), (0, 0))
    row_point = shifted(coeffs, "ka", -1)
    row_source = jnp.mod(my_cycle + 1, cycle_size)
    plane_kets = shifted(coeffs, "ka", -row_devices)
    plane_source = jnp.mod(my_cycle + row_devices, cycle_size)
    opposite = shifted(coeffs, "ka", cycle_size // 2)
    targets_flat = neighbour.reshape(-1)
    shifts_flat = shift_id.reshape(-1)
    target_device = targets_flat // k_local
    target_lane = targets_flat - target_device * k_local
    ket_index = jnp.where(
        target_device == my_cycle,
        target_lane,
        jnp.where(
            target_device == row_source,
            k_local,
            jnp.where(
                target_device == plane_source,
                k_local + 1 + target_lane,
                2 * k_local + 1 + target_lane,
            ),
        ),
    )
    bra_index = jnp.arange(pair_count, dtype=jnp.int32) // vector_count
    picks = (
        shifts_flat[:, None] == jnp.arange(block_map.shape[0], dtype=jnp.int32)[None, :]
    ).astype(jnp.int32)
    relabel = jnp.sum(picks[:, :, None] * block_map[None, :, :], axis=1)
    dest_global = jnp.broadcast_to(jnp.arange(all_blocks, dtype=jnp.int32)[None, :], relabel.shape)
    source_slice = relabel // slab_blocks
    dest_slice = dest_global // slab_blocks
    source_local = relabel - source_slice * slab_blocks
    dest_local = dest_global - dest_slice * slab_blocks
    kets = jnp.pad(jnp.concatenate([coeffs, row_point, plane_kets, opposite], axis=0), pad_spec)
    own_source = lax.dynamic_slice_in_dim(relabel, my_slice * slab_blocks, slab_blocks, 1)
    self_place = jnp.where(
        own_source // slab_blocks == my_slice, own_source - my_slice * slab_blocks, slab_blocks
    )
    ket_self = kets[ket_index[:, None], self_place]
    ket_self = ket_self.reshape(k_local, vector_count, slab_blocks, 2, band_count, lane_width)
    local_terms = complex_intersection(
        coeffs[:, :, 0],
        coeffs[:, :, 1],
        ket_self[:, :, :, 0],
        ket_self[:, :, :, 1],
        "ksmw,kbsnw->kbmn",
    )
    sent_block, where_to = slot_plan(
        dest_slice, source_slice, dest_local, source_local, my_slice, slices, capacity, slab_blocks
    )
    payload = coeffs[bra_index[:, None], sent_block]
    owner = jnp.broadcast_to(ket_index[:, None], (pair_count, slices))
    blocks = lax.all_to_all(payload, "ga", split_axis=1, concat_axis=1, tiled=True)
    places_in = lax.all_to_all(where_to, "ga", split_axis=1, concat_axis=1, tiled=True)
    owners = lax.all_to_all(owner, "ga", split_axis=1, concat_axis=1, tiled=True)
    partner = kets[owners[:, 0][:, None], places_in]
    remote = complex_intersection(
        blocks[:, :, 0], blocks[:, :, 1], partner[:, :, 0], partner[:, :, 1], "ismw,isnw->imn"
    )
    summed_part = local_terms + remote.reshape(k_local, vector_count, 2, band_count, band_count)
    total = lax.psum(summed_part, "ga")
    row_count = band_count // slices
    return lax.dynamic_slice_in_dim(total, my_slice * row_count, row_count, 3)


def gather_kernel(count, index_ref, source_ref, out_ref, sems):
    def copy(i):
        return pltpu.make_async_copy(source_ref.at[index_ref[i]], out_ref.at[i], sems.at[i])

    def begin(i, carry):
        copy(i).start()
        return carry

    def finish(i, carry):
        copy(i).wait()
        return carry

    lax.fori_loop(0, count, begin, 0)
    lax.fori_loop(0, count, finish, 0)


def gather_blocks(index, source):
    count = index.shape[0]
    shape = (count,) + source.shape[1:]
    return pl.pallas_call(
        functools.partial(gather_kernel, count),
        out_shape=jax.ShapeDtypeStruct(shape, source.dtype),
        in_specs=[
            pl.BlockSpec(memory_space=pltpu.SMEM),
            pl.BlockSpec(memory_space=pl.ANY),
        ],
        out_specs=pl.BlockSpec(memory_space=pltpu.VMEM),
        scratch_shapes=[pltpu.SemaphoreType.DMA((count,))],
        name="gather_blocks",
        cost_estimate=pl.CostEstimate(flops=0, bytes_accessed=4 * source.dtype.itemsize * count * source[0].size, transcendentals=0),
    )(index, source)


def plan_kernel(slab, capacity, shift_ref, map_ref, local_ref, sent_ref, got_ref):
    mine = lax.axis_index("ga")
    base = mine * slab
    for e in range(4):
        shift = shift_ref[e]

        def here(j, counts):
            own, out = counts
            source = map_ref[shift, base + j] - base
            inside = (source >= 0) & (source < slab)
            local_ref[0, e, own] = j
            local_ref[1, e, own] = source
            sent_ref[e, out] = j
            return own + inside.astype(jnp.int32), out + 1 - inside.astype(jnp.int32)

        def there(j, count):
            source = map_ref[shift, slab - base + j] - base
            inside = (source >= 0) & (source < slab)
            got_ref[e, count] = source
            return count + inside.astype(jnp.int32)

        lax.fori_loop(0, slab, here, (jnp.int32(0), jnp.int32(0)), unroll=8)
        lax.fori_loop(0, slab, there, jnp.int32(0), unroll=8)


def plan(shifts, block_map, slab, capacity):
    own_count = slab - capacity
    return pl.pallas_call(
        functools.partial(plan_kernel, slab, capacity),
        out_shape=(
            jax.ShapeDtypeStruct((2, 4, own_count + 8), jnp.int32),
            jax.ShapeDtypeStruct((4, capacity + 8), jnp.int32),
            jax.ShapeDtypeStruct((4, capacity + 8), jnp.int32),
        ),
        in_specs=[pl.BlockSpec(memory_space=pltpu.SMEM)] * 2,
        out_specs=[pl.BlockSpec(memory_space=pltpu.SMEM)] * 3,
        name="plan",
    )(shifts, block_map)


def meet_kernel(
    points, slab, capacity, local_ref, other_ref, send_ref, own_hbm, mine_out, out_ref,
    own, upper, lower, nxt, got_own, lower_out, got_lower, local_sems, send_sems, recv_sems,
):
    row = points // 4
    me = lax.axis_index("ka")
    partner = 1 - lax.axis_index("ga")
    z, column = me // row, me % row
    even = column % 2 == 0
    middle = (z == 1) | (z == 2)
    holds_pair = middle
    below = {"ka": (me + points - row) % points}
    above = {"ka": (me + row) % points}
    left = {"ka": z * row + (column + row - 1) % row}
    right = {"ka": z * row + (column + 1) % row}
    across = {"ga": partner}
    bands, lanes = own.shape[2], own.shape[3]
    size = slab // CHUNKS
    own_count = slab - capacity

    barrier = pltpu.get_barrier_semaphore()
    for peer in (below, above, left, right, across):
        pl.semaphore_signal(barrier, inc=1, device_id=peer, device_id_type=pl.DeviceIdType.MESH)
    pl.semaphore_wait(barrier, 5)

    def remote(source, target, n, peer):
        return pltpu.make_async_remote_copy(
            src_ref=source, dst_ref=target, send_sem=send_sems.at[n], recv_sem=recv_sems.at[n],
            device_id=peer, device_id_type=pl.DeviceIdType.MESH,
        )

    def chunk(c):
        return pl.ds(c * size, size)

    keep = pltpu.make_async_copy(own_hbm, own, local_sems.at[0])
    swap_own = remote(mine_out, got_own, 0, across)
    swap_lower = remote(lower_out, got_lower, 1, across)
    rise = [remote(own_hbm.at[chunk(c)], lower.at[chunk(c)], 2 + c, above) for c in range(CHUNKS)]
    fall = [remote(own_hbm.at[chunk(c)], upper.at[chunk(c)], 2 + CHUNKS + c, below) for c in range(CHUNKS)]
    pass_own = [remote(own_hbm.at[chunk(c)], nxt.at[chunk(c)], 2 + 2 * CHUNKS + c, left) for c in range(CHUNKS)]
    pass_on = [remote(upper.at[chunk(c)], nxt.at[chunk(c)], 2 + 2 * CHUNKS + c, left) for c in range(CHUNKS)]

    falls = even | (z >= 2)
    rises = ~even | (z <= 1)
    gets_upper = even | middle
    gets_lower = ~even | middle

    keep.start()
    swap_own.start()
    for c in range(CHUNKS):

        @pl.when(even & rises)
        def _():
            rise[c].start()

        @pl.when(~even & falls)
        def _():
            fall[c].start()

    for c in range(CHUNKS):

        @pl.when(column > 0)
        def _():
            pass_own[c].start()

        @pl.when(even)
        def _():
            fall[c].start()

        @pl.when(~even)
        def _():
            rise[c].start()

    def pick(ref, at):
        return ref[at].reshape(2 * bands, lanes)

    def product(total, first_left, second_left, first_right, second_right):
        return total + lax.dot_general(
            jnp.concatenate([first_left, second_left], axis=1),
            jnp.concatenate([first_right, second_right], axis=1),
            (((1,), (1,)), ((), ())),
            preferred_element_type=jnp.float32,
        )

    def edge(e, bra, ket, got, got_at, bra_sent):
        def own_step(i, total):
            for u in range(0, 10, 2):
                n = i * 10 + u
                total = product(
                    total,
                    pick(bra, local_ref[0, e, n]), pick(bra, local_ref[0, e, n + 1]),
                    pick(ket, local_ref[1, e, n]), pick(ket, local_ref[1, e, n + 1]),
                )
            return total

        def cross_step(i, total):
            n = i * 2
            travelled = pick(got, got_at + n), pick(got, got_at + n + 1)
            stayed_ref = ket if bra_sent else bra
            stayed = pick(stayed_ref, other_ref[e, n]), pick(stayed_ref, other_ref[e, n + 1])
            if bra_sent:
                return product(total, *travelled, *stayed)
            return product(total, *stayed, *travelled)

        total = jnp.zeros((2 * bands, 2 * bands), jnp.float32)
        total = lax.fori_loop(0, own_count // 10, own_step, total)
        total = lax.fori_loop(0, capacity // 2, cross_step, total)
        out_ref[e, 0] = total[:bands, :bands] + total[bands:, bands:]
        out_ref[e, 1] = total[:bands, bands:] - total[bands:, :bands]

    keep.wait()
    swap_own.wait_recv()

    def next_edge():
        for copy in pass_own:
            copy.wait_recv()
        edge(0, own, nxt, got_own, 0, True)

    @pl.when(column < row - 1)
    def _():
        next_edge()

    @pl.when(gets_upper)
    def _():
        for copy, onward in zip(fall, pass_on):
            copy.wait_recv()

            @pl.when(column == 0)
            def _():
                onward.start()

    @pl.when(gets_lower)
    def _():
        for copy in rise:
            copy.wait_recv()

    @pl.when(holds_pair)
    def _():
        def gather(r, carry):
            lower_out[r] = lower[send_ref[r]]
            return carry

        lax.fori_loop(0, 2 * capacity, gather, 0)
        swap_lower.start()

    @pl.when(even)
    def _():
        edge(1, own, upper, got_own, capacity, True)

    @pl.when(~even)
    def _():
        edge(1, lower, own, got_own, capacity, False)

    @pl.when(column == row - 1)
    def _():
        next_edge()

    @pl.when(holds_pair)
    def _():
        swap_lower.wait_recv()
        edge(2, lower, upper, got_lower, 0, True)
        edge(3, upper, lower, got_lower, capacity, False)
        swap_lower.wait_send()

    @pl.when(~holds_pair)
    def _():
        out_ref[2] = jnp.zeros_like(out_ref[2])
        out_ref[3] = jnp.zeros_like(out_ref[3])

    swap_own.wait_send()

    @pl.when(falls)
    def _():
        for copy in fall:
            copy.wait_send()

    @pl.when(rises)
    def _():
        for copy in rise:
            copy.wait_send()

    @pl.when(column > 0)
    def _():
        for copy in pass_own:
            copy.wait_send()

    @pl.when(column == 0)
    def _():
        for copy in pass_on:
            copy.wait_send()


def meet(local, other, send, own, mine_out, points, capacity):
    slab, bands = own.shape[0], own.shape[2]
    block = own.shape[1:]
    copies = 2 + 3 * CHUNKS
    return pl.pallas_call(
        functools.partial(meet_kernel, points, slab, capacity),
        out_shape=jax.ShapeDtypeStruct((4, 2, bands, bands), jnp.float32),
        in_specs=[pl.BlockSpec(memory_space=pltpu.SMEM)] * 3 + [pl.BlockSpec(memory_space=pl.ANY)] * 2,
        out_specs=pl.BlockSpec(memory_space=pltpu.VMEM),
        scratch_shapes=[pltpu.VMEM((slab,) + block, own.dtype)] * 4
        + [pltpu.VMEM((2 * capacity,) + block, own.dtype)] * 3
        + [pltpu.SemaphoreType.DMA((1,)), pltpu.SemaphoreType.DMA((copies,)), pltpu.SemaphoreType.DMA((copies,))],
        compiler_params=pltpu.CompilerParams(
            collective_id=0, has_side_effects=True, vmem_limit_bytes=32 * 2**20
        ),
        name="meet",
    )(local, other, send, own, mine_out)


def on_four_rows(coeffs, neighbour, shift_id, block_map):
    own = coeffs[0]
    slab = own.shape[0]
    points = lax.axis_size("ka")
    row = points // 4
    me = lax.axis_index("ka")
    first = lax.axis_index("ga") == 0
    even = jnp.mod(jnp.mod(me, row), 2) == 0
    capacity = 2 * max(1, slab // 12)
    to_lower = [((k + row) % points, k) for k in range(points)]
    to_upper = [((k - row) % points, k) for k in range(points)]
    swap = [(0, 1), (1, 0)]

    def role_shift(step):
        return jnp.sum(jnp.where(neighbour[0] == jnp.mod(me + step, points), shift_id[0], 0))

    row_shift, half_shift = role_shift(row), role_shift(points // 2)
    sent = jnp.stack([row_shift, half_shift])
    lower = lax.ppermute(sent, "ka", to_upper)
    upper = lax.ppermute(sent, "ka", to_lower)
    shifts = jnp.stack([role_shift(1), jnp.where(even, row_shift, lower[0]), lower[1], upper[1]])

    local, bras, kets = plan(shifts, block_map, slab, capacity)
    bras, kets = bras[:, :capacity], kets[:, :capacity]
    sends_bra = jnp.stack([even | True, even, even | True, even & False])[:, None]
    send = jnp.where(sends_bra, bras, kets)
    other = jnp.where(sends_bra, kets, bras)
    mine_out = gather_blocks(send[:2].reshape(-1), own)
    sums = meet(local, other, send[2:].reshape(-1), own, mine_out, points, capacity)

    half = sums.shape[2] // 2
    low_rows, high_rows = sums[:, :, :half], sums[:, :, half:]
    kept = jnp.where(first, low_rows, high_rows)
    total = kept + lax.ppermute(jnp.where(first, high_rows, low_rows), "ga", swap)
    from_upper = lax.ppermute(total[1:3], "ka", to_lower)
    from_lower = lax.ppermute(total[3], "ka", to_upper)
    row_sum = jnp.where(even, total[1], from_upper[0])
    half_sum = from_upper[1] + from_lower
    target = neighbour[0][:, None, None, None]
    out = jnp.where(
        target == jnp.mod(me + 1, points),
        total[0],
        jnp.where(target == jnp.mod(me + row, points), row_sum, half_sum),
    )
    return out[None]


def solution(mesh):
    in_specs = (P("ka", "ga", None, None, None), P("ka", None), P("ka", None), P())
    out_specs = P("ka", None, None, "ga", None)
    four_rows = mesh.shape["ga"] == 2 and mesh.shape["ka"] == 4 * min(16, mesh.shape["ka"] // 4)

    def run(coeffs, neighbour, shift_id, block_map):
        one_each = coeffs.shape[0] == mesh.shape["ka"]
        per_slice = coeffs.shape[1] // mesh.shape["ga"]
        whole_chunks = per_slice % (2 * CHUNKS) == 0 or per_slice % CHUNKS == 0 and per_slice % 2 == 0
        body = on_four_rows if four_rows and one_each and whole_chunks else on_device
        return jax.shard_map(
            body, mesh=mesh, in_specs=in_specs, out_specs=out_specs, check_vma=False
        )(coeffs, neighbour, shift_id, block_map)

    return run
```
